32 devices in a mesh: left: 8 (over z, x), right: 4 (over y, core).
Axes of the slice: x: 2, y: 2, z: 4, core: 2. Of those that a mesh axis runs over, the one named last changes fastest.
Arguments:
- species: float32 [4, 256, 128, 128], P(None, None, 'left', 'right'), may hold values from -6 to 6
- coupling: float32 [4, 4], replicated, may hold values from -4 to 4
- symbol_x: float32 [256], replicated, may hold values from 0.3 to 3
- symbol_y: float32 [128], replicated, may hold values from 0.3 to 3
- symbol_z: float32 [128], replicated, may hold values from 0.3 to 3
Outputs:
- modes: float32 [4, 256, 128, 128], P(None, 'left', 'right')
The draws below stay inside these ranges and needn't reach their ends.
All inputs are finite; a program needn't handle non-finite values.
Results may differ from the reference program's by a relative error of at most 0.000071.
Values sent between devices are 32-bit elements; how exact they have to be, the bound alone decides.
No kernel may reach another device: no remote copies, remote signals or barrier semaphores. Data moves between devices by JAX's collectives and lax.ppermute only.
A program may use at most 128 MiB of HBM per device.

```python
import jax
import jax.numpy as jnp
from jax import lax

GRID_X = 256
GRID_Y = 128
GRID_Z = 128
FIELDS = 4


def block_scale(stream_key, dims, pieces, smallest, top_value):
    def one(position, blocks):
        draws = jax.random.uniform(jax.random.fold_in(jax.random.fold_in(stream_key, 6), position), (blocks,), jnp.float32, smallest / len(pieces), top_value / len(pieces))
        return jnp.repeat(jnp.exp(draws), dims[position] // blocks).reshape((-1,) + (1,) * (len(dims) - position - 1))

    level = one(*pieces[0])
    for cut in pieces[1:]:
        level = level * one(*cut)
    return level


def noise(own_key, dims, deviation, reach, cuts=(), dtype=jnp.bfloat16):
    gain = block_scale(own_key, dims, cuts, -0.22, 0.18) if cuts else 1.0
    array = jax.random.normal(own_key, dims, jnp.float32) * deviation * gain
    return jnp.minimum(jnp.maximum(array, -reach), reach).astype(dtype)


def setup_inputs(seed: int = 0) -> dict:
    streams_of = jax.random.split(jax.random.key(seed), 6)
    species = noise(streams_of[0], (FIELDS, GRID_X, GRID_Y, GRID_Z), 1.0, 6.0, ((2, 8), (3, 4)), jnp.float32)
    coupling = noise(streams_of[1], (FIELDS, FIELDS), 0.7, 4.0, (), jnp.float32)
    symbol_x = jnp.clip(jax.random.uniform(streams_of[2], (GRID_X,), jnp.float32, 0.3, 3.0), 0.3, 3.0)
    symbol_y = jnp.clip(jax.random.uniform(streams_of[3], (GRID_Y,), jnp.float32, 0.3, 3.0), 0.3, 3.0)
    symbol_z = jnp.clip(jax.random.uniform(streams_of[4], (GRID_Z,), jnp.float32, 0.3, 3.0), 0.3, 3.0)
    return {"species": species, "coupling": coupling, "symbol_x": symbol_x, "symbol_y": symbol_y, "symbol_z": symbol_z}


def basis_table(count):
    rank = jnp.arange(count)
    angle = (2.0 * jnp.pi / count) * ((rank[:, None] * rank[None, :]) % count).astype(jnp.float32)
    return (jnp.cos(angle) + jnp.sin(angle)) * (count ** -0.5)


def along_dim(values, dim):
    moved = jnp.tensordot(values, basis_table(values.shape[dim]), axes=([dim], [0]), precision=lax.Precision.HIGHEST)
    return jnp.moveaxis(moved, -1, dim)


def reference(species, coupling, symbol_x, symbol_y, symbol_z):
    modes = species
    modes = along_dim(modes, 1)
    modes = along_dim(modes, 2)
    modes = along_dim(modes, 3)
    symbol = symbol_x[:, None, None] + symbol_y[None, :, None] + symbol_z[None, None, :]
    weight_xyz = 1.0 / (1.0 + symbol)
    mixed_fields = jnp.einsum("ab,bxyz->axyz", coupling, modes, precision=lax.Precision.HIGHEST)
    modes = weight_xyz * modes + (1.0 - weight_xyz) * mixed_fields
    return modes
```

```python
import functools

import jax
import jax.numpy as jnp
import numpy as np
from jax import lax
from jax.experimental import pallas as pl
from jax.experimental.pallas import tpu as pltpu
from jax.sharding import PartitionSpec as P

LANES = 128
SUBLANES = 8
CHUNKS = (4, 4)


def basis_halves(count):
    rank = np.arange(count)
    angle = 2.0 * np.pi / count * (rank[:, None] * rank[None, :] % count)
    table = ((np.cos(angle) + np.sin(angle)) * count ** (-0.5)).astype(np.float32)
    high = table.astype(jnp.bfloat16)
    low = (table - high.astype(np.float32)).astype(jnp.bfloat16)
    return high, low


def split(values):
    high = values.astype(jnp.bfloat16)
    low = (values - high.astype(jnp.float32)).astype(jnp.bfloat16)
    return high, low


def dot(left, right, right_dim=0):
    return lax.dot_general(
        left, right, (((1,), (right_dim,)), ((), ())), preferred_element_type=jnp.float32
    )


def swap(tiles, axis, step):
    tiles = list(tiles)
    size = tiles[0].shape[axis]
    place = lax.broadcasted_iota(jnp.int32, tiles[0].shape, axis) // step
    bit = len(tiles) // 2
    while bit:
        keep = (place & bit) == 0
        shift = bit * step
        for i in range(len(tiles)):
            if i & bit:
                continue
            one, two = tiles[i], tiles[i + bit]
            tiles[i] = jnp.where(keep, one, pltpu.roll(two, shift, axis))
            tiles[i + bit] = jnp.where(keep, pltpu.roll(one, size - shift, axis), two)
        bit //= 2
    return tiles


def x_kernel(chunks, lefts, place_ref, x_ref, high_ref, low_ref, *refs):
    outs, product = refs[:-1], refs[-1]
    me = place_ref[0]
    block = high_ref.shape[0] // lefts
    groups = block // SUBLANES
    size_y = x_ref.shape[1] // (LANES // groups)

    def rows(ref):
        return jnp.concatenate(
            [ref[pl.ds(pl.multiple_of((me ^ d) * block, block), block), :] for d in range(lefts)], axis=0
        )

    high, low = rows(high_ref), rows(low_ref)
    x_high, x_low = split(x_ref[0])
    product[...] = dot(high, x_high, 1) + dot(low, x_high, 1) + dot(high, x_low, 1)
    for d in range(lefts):
        lines = []
        for tile in range(size_y // groups):
            lines += swap(
                [
                    product[pl.ds(d * block + g * SUBLANES, SUBLANES), pl.ds(tile * LANES, LANES)]
                    for g in range(groups)
                ],
                1,
                LANES // groups,
            )
        for part in range(size_y // SUBLANES):
            turned = swap(lines[part * SUBLANES : (part + 1) * SUBLANES], 0, 1)
            first = 0
            for c, count in enumerate(chunks):
                for s in range(count):
                    outs[c * lefts + d][0, s, pl.ds(part * SUBLANES, SUBLANES), :] = turned[first + s]
                first += count


def y_kernel(lefts, rights, place_ref, high_ref, low_ref, *refs):
    parts, outs, lines = refs[:lefts], refs[lefts : lefts + rights], refs[-1]
    me_left, me_right = place_ref[0], place_ref[1]
    fields, count, share = parts[0].shape[:3]
    full = share * lefts
    for d in range(lefts):
        row = pl.multiple_of((me_left ^ d) * share, share)
        for f in range(fields):
            for s in range(count):
                high, low = split(parts[d][f, s])
                lane = pl.ds((f * count + s) * LANES, LANES)
                lines[pl.ds(row, share), lane] = high
                lines[pl.ds(full + row, share), lane] = low
    block = full // rights

    def rows(ref):
        return jnp.concatenate(
            [ref[pl.ds(pl.multiple_of((me_right ^ e) * block, block), block), :] for e in range(rights)], axis=0
        )

    high, low = rows(high_ref), rows(low_ref)
    both = jnp.concatenate([high, high], axis=1)
    for f in range(fields):
        lane = pl.ds(f * count * LANES, count * LANES)
        product = dot(both, lines[:, lane]) + dot(low, lines[pl.ds(0, full), lane])
        for s in range(count):
            for e in range(rights):
                outs[e][f, s] = product[e * block : (e + 1) * block, s * LANES : (s + 1) * LANES]


def z_kernel(rights, first, place_ref, coupling_ref, sx_ref, sy_ref, sz_ref, high_ref, low_ref, *refs):
    parts, out_ref = refs[:rights], refs[-1]
    me_left, me_right = place_ref[0], place_ref[1]
    fields, groups, _, share, _ = out_ref.shape
    size = LANES // groups
    halves = rights // groups

    def rows(ref):
        return jnp.concatenate(
            [ref[pl.ds(pl.multiple_of((me_right ^ e) * size, size), size), :] for e in range(rights)], axis=0
        )

    high, low = rows(high_ref), rows(low_ref)
    full = high.shape[1]
    table = jnp.concatenate(
        [jnp.concatenate([high, low], axis=1), jnp.concatenate([high, jnp.zeros_like(low)], axis=1)], axis=0
    )
    wide = (share, sy_ref.shape[1])
    here = lax.broadcasted_iota(jnp.int32, wide, 1) == lax.broadcasted_iota(jnp.int32, wide, 0) + me_right * share
    column = jnp.sum(jnp.where(here, sy_ref[...], 0.0), axis=1, keepdims=True)
    base = 1.0 + column + sz_ref[...]
    s = pl.program_id(0) + first
    old = []
    for f in range(fields):
        pieces = []
        for half in range(halves):
            pieces.append(swap([parts[half * groups + e][f, 0] for e in range(groups)], 1, size))
        line = jnp.concatenate(
            [jnp.concatenate([piece[g] for piece in pieces], axis=1) for g in range(groups)], axis=0
        )
        product = dot(jnp.concatenate(split(line), axis=1), table)
        old.append(product[:, :full] + product[:, full:])
    for g in range(groups):
        weight = 1.0 / (base + sx_ref[me_left * (groups * SUBLANES) + g * SUBLANES + s])
        row = slice(g * share, (g + 1) * share)
        for a in range(fields):
            total = coupling_ref[a, 0] * old[0][row]
            for b in range(1, fields):
                total = total + coupling_ref[a, b] * old[b][row]
            out_ref[a, g, 0] = weight * old[a][row] + (1.0 - weight) * total


def body(lefts, rights, species, coupling, symbol_x, symbol_y, symbol_z):
    fields, size_x, share_y, share_z = species.shape
    size_y, size_z = share_y * lefts, share_z * rights
    block = size_x // lefts
    groups = LANES // share_z
    share_out = size_y // rights
    assert block == groups * SUBLANES and rights % groups == 0 and share_y % (2 * SUBLANES) == 0
    assert sum(CHUNKS) == SUBLANES
    lines_x = jnp.transpose(species, (0, 2, 3, 1)).reshape(fields, share_y * share_z, size_x)
    place = jnp.stack([lax.axis_index("left"), lax.axis_index("right")]).astype(jnp.int32)
    smem = pl.BlockSpec(memory_space=pltpu.SMEM)
    vmem = pl.BlockSpec(memory_space=pltpu.VMEM)

    x_high, x_low = basis_halves(size_x)
    y_high, y_low = basis_halves(size_y)
    z_high, z_low = basis_halves(size_z)

    sent = pl.pallas_call(
        functools.partial(x_kernel, CHUNKS, lefts),
        grid=(fields,),
        in_specs=[
            smem,
            pl.BlockSpec((1, share_y * share_z, size_x), lambda f: (f, 0, 0)),
            pl.BlockSpec((size_x, size_x), lambda f: (0, 0)),
            pl.BlockSpec((size_x, size_x), lambda f: (0, 0)),
        ],
        out_specs=[
            pl.BlockSpec((1, count, share_y, LANES), lambda f: (f, 0, 0, 0)) for count in CHUNKS for _ in range(lefts)
        ],
        out_shape=[
            jax.ShapeDtypeStruct((fields, count, share_y, LANES), jnp.float32)
            for count in CHUNKS
            for _ in range(lefts)
        ],
        scratch_shapes=[pltpu.VMEM((size_x, share_y * share_z), jnp.float32)],
        name="x_lines",
    )(place, lines_x, x_high, x_low)

    result = None
    first = 0
    for c, count in enumerate(CHUNKS):
        mine = sent[c * lefts : (c + 1) * lefts]
        parts = [mine[0]] + [None] * (lefts - 1)
        for d in range(lefts - 1, 0, -1):
            parts[d] = lax.ppermute(mine[d], "left", [(k, k ^ d) for k in range(lefts)])
        turned = pl.pallas_call(
            functools.partial(y_kernel, lefts, rights),
            in_specs=[smem] + [vmem] * (2 + lefts),
            out_specs=[vmem] * rights,
            out_shape=[jax.ShapeDtypeStruct((fields, count, share_out, LANES), jnp.float32)] * rights,
            scratch_shapes=[pltpu.VMEM((2 * size_y, fields * count * LANES), jnp.bfloat16)],
            name=f"y_lines_{c}",
        )(place, y_high, y_low, *parts)
        parts = [turned[0]] + [None] * (rights - 1)
        for e in range(rights - 1, 0, -1):
            parts[e] = lax.ppermute(turned[e], "right", [(k, k ^ e) for k in range(rights)])
        shape = (fields, groups, SUBLANES, share_out, size_z)
        before = [] if result is None else [result]
        whole = lambda i: (0, 0)
        in_specs = [smem, smem, smem]
        in_specs += [pl.BlockSpec((1, size_y), whole), pl.BlockSpec((1, size_z), whole)]
        in_specs += [pl.BlockSpec((size_z, size_z), whole)] * 2
        in_specs += [pl.BlockSpec((fields, 1, share_out, LANES), lambda i: (0, i, 0, 0))] * rights
        result = pl.pallas_call(
            functools.partial(z_kernel, rights, first),
            grid=(count,),
            in_specs=in_specs + [pl.BlockSpec(memory_space=pl.ANY)] * len(before),
            out_specs=pl.BlockSpec(
                (fields, groups, 1, share_out, size_z), lambda i, first=first: (0, 0, i + first, 0, 0)
            ),
            out_shape=jax.ShapeDtypeStruct(shape, jnp.float32),
            input_output_aliases={len(in_specs): 0} if before else {},
            name=f"z_lines_{c}",
        )(
            place, coupling, symbol_x, symbol_y.reshape(1, size_y), symbol_z.reshape(1, size_z), z_high, z_low,
            *parts, *before,
        )
        first += count
    return result.reshape(fields, block, share_out, size_z)


def solution(mesh):
    in_specs = (P(None, None, "left", "right"), P(), P(), P(), P())
    out_specs = P(None, "left", "right", None)
    step = functools.partial(body, mesh.shape["left"], mesh.shape["right"])
    return jax.shard_map(step, mesh=mesh, in_specs=in_specs, out_specs=out_specs, check_vma=False)
```
